32 devices in a mesh: adapter: 16 (over z, y, x), mp: 2 (over core).
Axes of the slice: x: 2, y: 2, z: 4, core: 2. Of those that a mesh axis runs over, the one named last changes fastest.
Arguments:
- hidden: bfloat16 [4096, 4096], P('adapter', 'mp'), may hold values from -8 to 8
- subsets: int32 [4096, 8], P('adapter'), may hold values from 0 to 15, all different within a row; in each aligned block of 256 rows (0 to 255, 256 to 511, ...) at most 256 rows name the same one
- down_weight: bfloat16 [16, 4096, 256], P('adapter', 'mp'), may hold values from -0.09375 to 0.09375
- up_weight: bfloat16 [16, 256, 4096], P('adapter', None, 'mp'), may hold values from -0.375 to 0.375
- query_weight: bfloat16 [4096, 4096], P('mp'), may hold values from -0.08 to 2.08
- key_weight: bfloat16 [4096, 4096], P('mp'), may hold values from -0.08 to 2.08
Outputs:
- joined: bfloat16 [4096, 4096], P('adapter', 'mp')
The draws below stay inside these ranges and needn't reach their ends.
Inputs may be any that keep to these rules, and one draw needn't show every extreme that they name: `subsets`: each row names 8 different adapters; within the rows of one index of the adapter axis no adapter is named by more than 256 rows.
All inputs are finite; a program needn't handle non-finite values.
Results may differ from the reference program's by a relative error of at most 0.025.
Values may be sent and summed in bfloat16 or wider, within the bound.
A program may use at most 192 MiB of HBM per device.

```python
import math
import jax
import jax.numpy as jnp
import numpy as np
from jax import lax

D = 4096
B = 256
K = 8
REQ_DEV = 256
ADAPTERS = 16
REQUESTS = 4096
CAP = 256


def draw_hidden(key, part):
    values = jnp.clip(jax.random.normal(key, (REQUESTS, D), jnp.float32), -5.0, 5.0)
    return values.astype(jnp.bfloat16)


def draw_query_weight(key, part):
    values = jnp.clip(jax.random.normal(jax.random.fold_in(key, 11), (D, D), jnp.float32) * D ** (-0.5), -0.078125, 0.078125)
    return values.astype(jnp.bfloat16)


def draw_key_weight(key, part):
    values = jnp.clip(jax.random.normal(jax.random.fold_in(key, 13), (D, D), jnp.float32) * D ** (-0.5), -0.078125, 0.078125)
    return values.astype(jnp.bfloat16)


def level_of(rng, extent, pieces, least, high):
    gain = 1.0
    for axis_at, parts in pieces:
        draws = jax.random.uniform(jax.random.fold_in(jax.random.fold_in(rng, 6), axis_at), (parts,), jnp.float32, least / len(pieces), high / len(pieces))
        gain = gain * jnp.repeat(jnp.exp(draws), extent[axis_at] // parts).reshape((-1,) + (1,) * (len(extent) - 1 - axis_at))
    return gain


def shared_out(stream_key, own, number, rows, count, top, reach, lean):
    ranking = jax.random.permutation(stream_key, count)
    crowded, common = shares(count, rows * top, reach, lean, True), shares(count, rows * top, reach, lean, False)
    places = jnp.arange(count)

    def named(tallies, offset_by):
        used = int((tallies > 0).sum())
        fixed = max(1, used // 4)
        moved = fixed + (places - fixed + offset_by * (used - fixed)) % max(1, count - fixed)
        return jnp.zeros((count,), jnp.int32).at[ranking[jnp.where(places < fixed, places, moved)]].set(jnp.asarray(tallies, jnp.int32))

    tallies = jnp.where(number % 4 == 0, named(crowded, number // 4), named(common, number - number // 4 - 1))
    mixed = jax.random.permutation(jax.random.fold_in(own, 3), count)
    source_of, receiver = mixed[0:count // 2 * 2:2], mixed[1:count // 2 * 2:2]
    slack = jnp.minimum(tallies[source_of] - 1, reach - tallies[receiver]) // 2
    slack = jnp.where((source_of == ranking[0]) | (receiver == ranking[0]) | (tallies[receiver] == 0), 0, jnp.maximum(slack, 0))
    moved = jax.random.randint(jax.random.fold_in(own, 4), (count // 2,), 0, 1 << 20) % (slack + 1)
    tallies = tallies.at[source_of].add(-moved).at[receiver].add(moved)
    items = jnp.searchsorted(jnp.cumsum(tallies), jnp.arange(rows * top), side="right").astype(jnp.int32)
    table = items.reshape(top, rows).T
    table = table[jax.random.permutation(jax.random.fold_in(own, 1), rows)]
    offset_by = jax.random.randint(jax.random.fold_in(own, 2), (rows, 1), 0, top)
    return jnp.take_along_axis(table, (jnp.arange(top)[None, :] + offset_by) % top, axis=1)


def shares(number_of, total, bound, slope, full):
    weights = [(1 << 20) // math.isqrt(rank ** slope) + 1 for rank in range(1, number_of + 1)]
    largest = bound if full else min(bound, max(-(-total // number_of), total * weights[0] // sum(weights)))
    least = 1 if total - largest >= number_of - 1 else 0
    counts, surplus = [largest] + [least] * (number_of - 1), total - largest - least * (number_of - 1)
    while surplus > 0:
        candidates = [i for i in range(1, number_of) if counts[i] < largest] or [i for i in range(1, number_of) if counts[i] < bound]
        mass, left = sum([weights[i] for i in candidates]), surplus
        for i in candidates:
            extra = min(bound - counts[i], max(1, left * weights[i] // mass), surplus)
            counts[i] = counts[i] + extra
            surplus = surplus - extra
    return np.array(counts)


def bell_draw(rng, extent, spread, limit, pieces=(), kind=jnp.bfloat16):
    result = spread * jax.random.normal(rng, extent, jnp.float32)
    if pieces:
        result = result * level_of(rng, extent, pieces, -0.22, 0.18)
    return jnp.clip(result, -limit, limit).astype(kind)


def setup_inputs(seed: int = 0) -> dict:
    seeds = jax.random.split(jax.random.key(seed), 7)
    hidden = draw_hidden(jax.random.fold_in(seeds[6], 71), 0)
    subsets_keys = jax.random.split(jax.random.fold_in(seeds[1], 1), REQUESTS // REQ_DEV)
    subsets_turns = jax.random.permutation(jax.random.fold_in(seeds[1], 3), REQUESTS // REQ_DEV)
    subsets = jax.vmap(lambda own, number: shared_out(jax.random.fold_in(seeds[1], 2), own, number, REQ_DEV, ADAPTERS, K, CAP, 2))(subsets_keys, subsets_turns).reshape((REQUESTS, K))
    down_weight = bell_draw(seeds[2], (ADAPTERS, D, B), D ** -0.5, 0.09375, ((0, 16), (1, 2)))
    up_weight = bell_draw(seeds[3], (ADAPTERS, B, D), B ** -0.5, 0.375, ((0, 16), (2, 2)))
    query_weight = draw_query_weight(jax.random.fold_in(seeds[6], 71), 0)
    key_weight = draw_key_weight(jax.random.fold_in(seeds[6], 71), 0)
    return dict(hidden=hidden, subsets=subsets, down_weight=down_weight, up_weight=up_weight, query_weight=query_weight, key_weight=key_weight)


def reference(hidden, subsets, down_weight, up_weight, query_weight, key_weight):
    query = jnp.dot(hidden, query_weight, preferred_element_type=jnp.float32).astype(jnp.bfloat16)
    probe = lax.dot_general(query, key_weight, (((1,), (1,)), ((), ())), preferred_element_type=jnp.float32).astype(jnp.bfloat16)

    def visit(gathered, operands):
        index, down_one, up_one = operands
        bottle = jnp.maximum(jnp.dot(hidden, down_one, preferred_element_type=jnp.float32), 0.0).astype(jnp.bfloat16)
        produced = jnp.dot(bottle, up_one, preferred_element_type=jnp.float32).astype(jnp.bfloat16)
        landed = subsets == index
        gathered = jnp.where(landed[:, :, None], produced[:, None, :], gathered)
        return gathered, None

    start_value = jnp.zeros((REQUESTS, K, D), jnp.bfloat16)
    picked, _ = lax.scan(visit, start_value, (jnp.arange(ADAPTERS, dtype=jnp.int32), down_weight, up_weight))
    widened = picked.astype(jnp.float32)
    base = hidden.astype(jnp.float32)
    probe_wide = probe.astype(jnp.float32)
    own_term = jnp.sum(base * probe_wide, axis=1)
    logits = (jnp.einsum("rkd,rd->rk", widened, probe_wide, precision=lax.Precision.HIGHEST) + own_term[:, None]) * (D ** -0.5)
    share = jax.nn.softmax(logits, axis=-1)
    joined = base + jnp.einsum("rk,rkd->rd", share, widened, precision=lax.Precision.HIGHEST)
    return joined.astype(jnp.bfloat16)
```

```python
import jax
import jax.numpy as jnp
import numpy as np
from jax import lax
from jax.sharding import PartitionSpec as P


def both_cores(part):
    size = lax.axis_size("mp")
    total = part
    for shift in range(1, size):
        total = total + lax.ppermute(part, "mp", [(i, (i + shift) % size) for i in range(size)])
    return total


def per_device(hidden, subsets, down_weight, up_weight, query_weight, key_weight):
    n = lax.axis_size("adapter")
    rows, width = hidden.shape
    bottleneck = down_weight.shape[2]
    model_width = query_weight.shape[1]
    half = width // 2
    me = lax.axis_index("adapter")
    side, spot = me % 2, me // 2
    count = n // 2
    swap = [(i, i ^ 1) for i in range(n)]

    def swapped(array):
        return lax.ppermute(array, "adapter", swap)

    cycle = list(range(0, count, 2)) + list(range(1, count, 2))[::-1]
    down, up = down_weight[0], up_weight[0]

    def ring(order, held):
        place = {node: i for i, node in enumerate(order)}
        table = np.array(
            [[order[(place[node] - s) % count] for s in range(count)] for node in range(count)],
            np.int32,
        )
        hops = [
            (order[i] * 2 + x, order[(i + 1) % count] * 2 + x)
            for i in range(count)
            for x in range(2)
        ]
        owners = lax.dynamic_index_in_dim(jnp.asarray(table), spot, 0, keepdims=False)
        blocks = [held]
        for _ in range(1, count):
            blocks.append(lax.ppermute(blocks[-1], "adapter", hops))
        return blocks, owners

    both = jnp.concatenate([hidden, swapped(hidden)], axis=0)
    subset_both = jnp.concatenate([subsets, swapped(subsets)], axis=0)
    down_rings = [ring(cycle, down[:half]), ring(cycle[::-1], down[half:])]
    halves = [up[:, :half], up[:, half:]]
    up_rings = [ring(cycle, halves[0]), ring(cycle[::-1], halves[1])]

    query_part = jnp.dot(hidden, query_weight, preferred_element_type=jnp.float32)
    query = both_cores(query_part.astype(jnp.bfloat16))
    probe = lax.dot_general(
        query, key_weight, (((1,), (1,)), ((), ())), preferred_element_type=jnp.float32
    ).astype(jnp.bfloat16)
    probe = jnp.concatenate([probe, swapped(probe)], axis=0)
    own_term = jnp.sum(both.astype(jnp.float32) * probe.astype(jnp.float32), axis=1)

    def placed(buffer, block, owner):
        return lax.dynamic_update_slice(buffer, block[None], (owner, 0, 0))

    bottle_part, reach, ups = [], [], []
    for h in range(2):
        columns = slice(h * half, (h + 1) * half)
        blocks, owners = down_rings[h]
        total = jnp.zeros((count, 2 * rows, bottleneck), jnp.float32)
        for s in range(count):
            piece = jnp.dot(both[:, columns], blocks[s], preferred_element_type=jnp.float32)
            total = placed(total, piece, owners[s])
        bottle_part.append(total)
    for h in range(2):
        columns = slice(h * half, (h + 1) * half)
        blocks, owners = up_rings[h]
        total = jnp.zeros((count, 2 * rows, bottleneck), jnp.float32)
        kept = jnp.zeros((count, bottleneck, half), jnp.bfloat16)
        for s in range(count):
            piece = lax.dot_general(
                probe[:, columns],
                blocks[s],
                (((1,), (1,)), ((), ())),
                preferred_element_type=jnp.float32,
            )
            total = placed(total, piece, owners[s])
            kept = placed(kept, blocks[s], owners[s])
        reach.append(total)
        ups.append(kept.reshape(count * bottleneck, half))

    summed = both_cores((bottle_part[0] + bottle_part[1]).astype(jnp.bfloat16))
    wide = jnp.maximum(summed, 0).astype(jnp.float32)
    partial_logit = jnp.sum(wide * (reach[0] + reach[1]), axis=2) + own_term[None, :]
    logits = both_cores(partial_logit) * model_width ** (-0.5)
    theirs = swapped(logits)
    theirs = jnp.concatenate([theirs[:, rows:], theirs[:, :rows]], axis=1)

    def masked(values, parity):
        labels = 2 * jnp.arange(count, dtype=jnp.int32) + parity
        named = jnp.any(subset_both[None, :, :] == labels[:, None, None], axis=2)
        return jnp.where(named, values, -jnp.inf)

    share = jax.nn.softmax(
        jnp.concatenate([masked(logits, side), masked(theirs, 1 - side)], axis=0), axis=0
    )[:count]
    weighted = (wide * share[:, :, None]).astype(jnp.bfloat16)
    weighted = weighted.transpose(1, 0, 2).reshape(2 * rows, count * bottleneck)
    joined = []
    sent = [
        swapped(jnp.dot(weighted[rows:], u, preferred_element_type=jnp.float32).astype(jnp.bfloat16))
        for u in ups
    ]
    for h in range(2):
        own = jnp.dot(weighted[:rows], ups[h], preferred_element_type=jnp.float32)
        base = hidden[:, h * half : (h + 1) * half].astype(jnp.float32)
        joined.append((base + own + sent[h].astype(jnp.float32)).astype(jnp.bfloat16))
    return jnp.concatenate(joined, axis=1)


def solution(mesh):
    return jax.shard_map(
        per_device,
        mesh=mesh,
        in_specs=(
            P("adapter", "mp"),
            P("adapter", None),
            P("adapter", "mp", None),
            P("adapter", None, "mp"),
            P("mp", None),
            P("mp", None),
        ),
        out_specs=P("adapter", "mp"),
        check_vma=False,
    )
```
